128 devices in a mesh: view: 4 (over z_hi, core), depth: 32 (over z_lo, y, x).
Axes of the slice: x: 4, y: 4, z: 4 (z_hi: 2, z_lo: 2; z = z_hi * 2 + z_lo), core: 2. Of those that a mesh axis runs over, the one named last changes fastest.
Arguments:
- volume: float32 [512, 128, 2048], P(('view', 'depth')), may hold values from -6 to 6
- step_weights: float32 [4, 8, 64], P('view'), may hold values from -0.75 to 0.75
- row_interp: float32 [4, 64, 64], P('view'), may hold values from -0.75 to 0.75
- col_interp: float32 [4, 64, 64], P('view'), may hold values from -0.75 to 0.75
- tf_table: float32 [8, 8], replicated, may hold values from -3 to 3
- materials: int32 [8, 2, 32], P(None, None, 'depth'), may hold values from 0 to 7
- entry: int32 [4, 512, 128], P('view'), may hold values from 0 to 15
Outputs:
- picture: float32 [4, 3, 512, 128], P('view', None, 'depth')
The draws below stay inside these ranges and needn't reach their ends.
All inputs are finite; a program needn't handle non-finite values.
Results may differ from the reference program's by a relative error of at most 0.00018.
Values sent between devices are 32-bit elements; how exact they have to be, the bound alone decides.
A program may use at most 64 MiB of HBM per device.

```python
import jax
import jax.numpy as jnp
from jax import lax

BRICK = 64
STEPS_B = 8
MATS = 8
NY = 128
NZ = 512
NX = 2048
N_VIEW = 4
N_DEPTH = 32


def plant(result, stream_key, least, top_value):
    longest = result.shape.index(max(result.shape))
    spots = []
    for shift in (0, 1):
        where = [jax.random.randint(jax.random.fold_in(stream_key, axis), (), 0, length) for axis, length in enumerate(result.shape)]
        where[longest] = (where[longest] + shift) % result.shape[longest]
        spots.append(tuple(where))
    return result.at[spots[0]].set(least).at[spots[1]].set(top_value)


def steps_of(rng, dims, shards, low, largest):
    gain, own = 1.0, jax.random.fold_in(rng, 6)
    for axis_at, blocks in shards:
        heights = jnp.exp(jax.random.uniform(jax.random.fold_in(own, axis_at), (blocks,), jnp.float32, low / len(shards), largest / len(shards)))
        gain = gain * jnp.repeat(heights, dims[axis_at] // blocks).reshape([-1 if axis == axis_at else 1 for axis in range(len(dims))])
    return gain


def bell_draw(own_key, dims, scale, most, shards=(), kind=jnp.bfloat16):
    entries = scale * jax.random.normal(own_key, dims, jnp.float32)
    if shards:
        entries = entries * steps_of(own_key, dims, shards, -0.22, 0.18)
    return jnp.clip(entries, -most, most).astype(kind)


def setup_inputs(seed: int = 0) -> dict:
    arg_keys = jax.random.split(jax.random.key(seed), 8)
    volume = bell_draw(arg_keys[0], (NZ, NY, NX), 1.0, 6.0, ((0, 128),), jnp.float32)
    step_weights = bell_draw(arg_keys[1], (N_VIEW, STEPS_B, BRICK), BRICK ** -0.5, 0.75, ((0, 4),), jnp.float32)
    row_interp = bell_draw(arg_keys[2], (N_VIEW, BRICK, BRICK), BRICK ** -0.5, 0.75, ((0, 4),), jnp.float32)
    col_interp = bell_draw(arg_keys[3], (N_VIEW, BRICK, BRICK), BRICK ** -0.5, 0.75, ((0, 4),), jnp.float32)
    tf_table = bell_draw(arg_keys[4], (MATS, 8), 1.0, 3.0, (), jnp.float32)
    materials = plant(jax.random.randint(arg_keys[5], (NZ // BRICK, NY // BRICK, N_DEPTH), 0, MATS), jax.random.fold_in(arg_keys[5], 1), 0, MATS - 1).astype(jnp.int32)
    entry = plant(jax.random.randint(arg_keys[6], (N_VIEW, NZ, NY), 0, N_DEPTH // 2), jax.random.fold_in(arg_keys[6], 1), 0, (N_DEPTH // 2) - 1).astype(jnp.int32)
    return {"volume": volume, "step_weights": step_weights, "row_interp": row_interp, "col_interp": col_interp, "tf_table": tf_table, "materials": materials, "entry": entry}


def sample_brick(cells, steps_map, rows_map, cols_map):
    highest = lax.Precision.HIGHEST
    edge = rows_map.shape[0]
    first = jnp.einsum('zyi,si->szy', cells, steps_map, precision=highest)
    count_steps, total_rows, total_cols = first.shape
    second = first.reshape(count_steps, total_rows // edge, edge, total_cols)
    second = jnp.einsum('stky,rk->stry', second, rows_map, precision=highest)
    third = second.reshape(count_steps, total_rows, total_cols // edge, edge)
    third = jnp.einsum('szuj,cj->szuc', third, cols_map, precision=highest)
    return third.reshape(count_steps, total_rows, total_cols)


def expand_classes(classes, tf_table, edge):
    choices_range = jnp.arange(tf_table.shape[0], dtype=jnp.int32)
    onehot = (classes[:, :, None] == choices_range).astype(jnp.float32)
    tiles = jnp.einsum('abm,mc->cab', onehot, tf_table, precision=lax.Precision.HIGHEST)
    count_coef, tiles_rows, tiles_cols = tiles.shape
    spread = jnp.broadcast_to(tiles[:, :, None, :, None], (count_coef, tiles_rows, edge, tiles_cols, edge))
    return spread.reshape(count_coef, tiles_rows * edge, tiles_cols * edge)


def shade(samples, coefficients, live_mask, step_length):
    emission = jax.nn.softplus(coefficients[0:3, None] * samples[None] + coefficients[3:6, None])
    tau = step_length * live_mask[None] * jax.nn.softplus(coefficients[6][None] * samples + coefficients[7][None])
    earlier = jnp.cumsum(tau, axis=0) - tau
    weights = jnp.exp(-earlier) * (1.0 - jnp.exp(-tau))
    colours = jnp.sum(weights[None] * emission, axis=1)
    passed = jnp.exp(-jnp.sum(tau, axis=0))
    return colours, passed


def reference(volume, step_weights, row_interp, col_interp, tf_table, materials, entry):
    step_length = 2.0 / (STEPS_B * N_DEPTH)
    pictures = []
    for view_index in range(N_VIEW):
        picture = jnp.zeros((3, NZ, NY), jnp.float32)
        carried = jnp.ones((NZ, NY), jnp.float32)
        for depth_index in range(N_DEPTH):
            cells = volume[:, :, depth_index * BRICK:(depth_index + 1) * BRICK]
            samples = sample_brick(cells, step_weights[view_index], row_interp[view_index], col_interp[view_index])
            coefficients = expand_classes(materials[:, :, depth_index], tf_table, BRICK)
            live_mask = (entry[view_index] <= depth_index).astype(jnp.float32)
            colours, passed = shade(samples, coefficients, live_mask, step_length)
            picture = picture + carried[None] * colours
            carried = carried * passed
        pictures.append(picture)
    return jnp.stack(pictures)
```

```python
import jax
import jax.numpy as jnp
from jax import lax
from jax.experimental import pallas as pl
from jax.experimental.pallas import tpu as pltpu
from jax.sharding import Mesh
from jax.sharding import PartitionSpec as P

AXES = ("zh", "core", "zl", "y", "x")
VIEW = ("zh", "core")
DEPTH = ("zl", "y", "x")
MESH = pl.DeviceIdType.MESH
STEP_LENGTH = 2.0 / 256.0
BF16 = jnp.bfloat16
F32 = jnp.float32


def split(value):
    high = value.astype(BF16)
    low = (value - high.astype(F32)).astype(BF16)
    return high, low


def dot_nt(lhs, rhs):
    return lax.dot_general(lhs, rhs, (((1,), (1,)), ((), ())), preferred_element_type=F32)


def softplus(v):
    return jnp.maximum(v, 0.0) + jnp.log1p(jnp.exp(-jnp.abs(v)))


def step_block(weights):
    twice = jnp.concatenate([weights, weights], axis=1)
    lane = lax.broadcasted_iota(jnp.int32, twice.shape, 1)
    block = jnp.concatenate(
        [jnp.where(lane < 64, twice, 0.0), jnp.where(lane >= 64, twice, 0.0)], axis=0
    )
    high = block.astype(BF16).astype(F32)
    return high, block - high


def step_lhs(weights):
    parts = [step_block(one) for one in weights]
    high = jnp.concatenate([part[0] for part in parts], axis=0)
    low = jnp.concatenate([part[1] for part in parts], axis=0)
    top = jnp.concatenate([high, high], axis=1)
    bottom = jnp.concatenate([low, jnp.zeros_like(low)], axis=1)
    return jnp.concatenate([top, bottom], axis=0).astype(BF16)


def kernel(
    vol, own_w, rows_map, cols_map, table, mats, entry, out,
    cells, sent, got, other_w, row_buf, col_buf, entry_buf, coef_own, coefs,
    row_lhs, col_rhs, second, samples, part, finals,
    cell_sem, send_sem, got_sem, w_send, w_got, map_send, map_got,
    coef_send, coef_got, fin_send, fin_got,
):
    zh, core, zl = lax.axis_index("zh"), lax.axis_index("core"), lax.axis_index("zl")
    y, x = lax.axis_index("y"), lax.axis_index("x")
    place = y * 4 + x
    shift = lax.rem(y - 2 * core - zl + 8, 4)
    mine = lax.rem(2 + 3 * shift, 4)
    view_zh = lax.rem(zh + mine // 2, 2)
    view_core = lax.rem(core + lax.rem(mine, 2), 2)

    def device(zh_=zh, core_=core, zl_=zl, y_=y, x_=x):
        return {"zh": zh_, "core": core_, "zl": zl_, "y": y_, "x": x_}

    def remote(src, dst, send, recv, where):
        return pltpu.make_async_remote_copy(
            src_ref=src, dst_ref=dst, send_sem=send, recv_sem=recv,
            device_id=where, device_id_type=MESH,
        )

    def plane_peer(offset):
        return lax.rem(y + offset // 4, 4), lax.rem(x + lax.rem(offset, 4), 4)

    def view_peer(xor):
        return device(zh_=lax.rem(zh + xor // 2, 2), core_=lax.rem(core + xor % 2, 2))

    octet = zl * 2 + y // 2
    brick_slot = lax.rem(y, 2) * 4 + x
    coef_self = x == octet

    barrier = pltpu.get_barrier_semaphore()

    def greet(where):
        pl.semaphore_signal(barrier, inc=1, device_id=where, device_id_type=MESH)

    @pl.loop(1, 16)
    def _(offset):
        peer_y, peer_x = plane_peer(offset)
        greet(device(y_=peer_y, x_=peer_x))

    for xor in (1, 2, 3):
        greet(view_peer(xor))

    @pl.loop(0, 8)
    def _(i):
        to_zl, to_y = i // 4, lax.rem(i, 4)
        from_y, from_x = 2 * lax.rem(x, 2) + i // 4, lax.rem(i, 4)

        @pl.when(jnp.logical_not(coef_self & (to_zl == zl) & (to_y == y)))
        def _():
            greet(device(zl_=to_zl, y_=to_y, x_=octet))

        @pl.when(jnp.logical_not(coef_self & (from_y == y) & (from_x == x)))
        def _():
            greet(device(zl_=x // 2, y_=from_y, x_=from_x))

    out_y = 2 * core + zl
    source_zh, source_core, source_zl = zl, y // 2, lax.rem(y, 2)
    source_xor = lax.rem(zh + source_zh, 2) * 2 + lax.rem(core + source_core, 2)
    source_y = lax.rem(y + 2 + 3 * source_xor, 4)

    @pl.loop(0, 4)
    def _(i):
        greet(device(view_zh, view_core, zh, out_y, i))
        greet(device(source_zh, source_core, source_zl, source_y, i))

    def cell_copy(rho, q):
        return pltpu.make_async_copy(
            vol.at[:, :, pl.ds(512 * q + 128 * rho, 128)], cells.at[rho, q], cell_sem.at[rho, q]
        )

    for rho in range(4):
        for q in range(4):
            cell_copy(rho, q).start()

    def contract(lhs, rho, q, first_view, count):
        high, low = split(cells[rho, q].reshape(512, 128))
        wide = dot_nt(lhs, jnp.concatenate([high, low], axis=1))
        wide = wide[: 16 * count] + wide[16 * count :]
        for k in range(count):
            for pair in range(2):
                for z in range(4):
                    row = 16 * k + 8 * pair
                    sent[(first_view + k) * 4 + q, 2 * rho + pair, pl.ds(8 * z, 8), :] = wide[
                        row : row + 8, 128 * z : 128 * z + 128
                    ]

    def send_brick(j, offset):
        peer_y, peer_x = plane_peer(offset)
        peer_shift = lax.rem(peer_y - 2 * core - zl + 8, 4)
        slot = lax.rem(2 + 3 * peer_shift, 4) * 4 + peer_x
        return remote(
            sent.at[slot, j], got.at[j, pl.ds(32 * place, 32)], send_sem.at[0], got_sem.at[j],
            device(y_=peer_y, x_=peer_x),
        )

    def peer_xor(offset):
        peer_y, _ = plane_peer(offset)
        return lax.rem(2 + 3 * lax.rem(peer_y - 2 * core - zl + 8, 4), 4)

    own_lhs = step_lhs([own_w[0]])
    for rho in range(4):
        for q in range(4):
            cell_copy(rho, q).wait()
            contract(own_lhs, rho, q, 0, 1)

    lane = lax.broadcasted_iota(jnp.int32, (8, 128), 1)
    sublane = lax.broadcasted_iota(jnp.int32, (8, 128), 0)
    for k in range(2):
        tile = 2 * (2 * zh + core) + k
        wanted = jnp.where(lane < 64, mats[tile, 0, 0], mats[tile, 1, 0])
        onehot = (sublane == wanted).astype(F32)
        coef_own[k] = lax.dot_general(
            table[...], onehot, (((0,), (0,)), ((), ())),
            precision=lax.Precision.HIGHEST, preferred_element_type=F32,
        )

    @pl.when(coef_self)
    def _():
        coefs[brick_slot] = coef_own[zl]

    pl.semaphore_wait(barrier, 42 - 2 * coef_self.astype(jnp.int32))

    w_copies = [
        remote(own_w.at[0], other_w.at[xor], w_send.at[xor], w_got.at[xor], view_peer(xor))
        for xor in (1, 2, 3)
    ]
    for copy in w_copies:
        copy.start()

    @pl.loop(0, 8)
    def _(j):
        @pl.loop(1, 16)
        def _(offset):
            @pl.when(peer_xor(offset) == 0)
            def _():
                send_brick(j, offset).start()

    turned = lax.rem(shift, 2) == 1
    to_xor = jnp.where(turned, lax.rem(2 + 3 * (shift + 2), 4), mine)
    to_zh, to_core = lax.rem(zh + to_xor // 2, 2), lax.rem(core + lax.rem(to_xor, 2), 2)
    to_rows = pl.multiple_of((2 * (2 * to_zh + to_core) + zl) * 64, 64)
    to_device = device(zh_=to_zh, core_=to_core)
    maps = (
        (rows_map.at[0], row_buf),
        (cols_map.at[0], col_buf),
        (entry.at[0, pl.ds(to_rows, 64)], entry_buf),
    )

    @pl.when(mine == 0)
    def _():
        for i, (src, dst) in enumerate(maps):
            pltpu.make_async_copy(src, dst, map_got.at[i]).start()

    @pl.when(mine != 0)
    def _():
        for i, (src, dst) in enumerate(maps):
            remote(src, dst, map_send.at[i], map_got.at[i], to_device).start()

    def coef_copy(i):
        to_zl, to_y = i // 4, lax.rem(i, 4)
        return remote(
            coef_own.at[to_zl], coefs.at[brick_slot], coef_send.at[0], coef_got.at[0],
            device(zl_=to_zl, y_=to_y, x_=octet),
        )

    @pl.loop(0, 8)
    def _(i):
        @pl.when(jnp.logical_not(coef_self & (i // 4 == zl) & (lax.rem(i, 4) == y)))
        def _():
            coef_copy(i).start()

    for copy in w_copies:
        copy.wait()
    lhs = step_lhs([other_w[1], other_w[2], other_w[3]])
    for rho in range(4):
        for q in range(4):
            contract(lhs, rho, q, 1, 3)

        for pair in range(2):
            @pl.loop(1, 16)
            def _(offset, j=2 * rho + pair):
                @pl.when(peer_xor(offset) != 0)
                def _():
                    send_brick(j, offset).start()

    own_slot = mine * 4 + x

    @pl.loop(0, 8)
    def _(j):
        got[j, pl.ds(pl.multiple_of(32 * place, 32), 32), :] = sent[own_slot, j]

    for i, (src, dst) in enumerate(maps):
        pltpu.make_async_copy(src, dst, map_got.at[i]).wait()

    row_map = row_buf[...]
    row_high = row_map.astype(BF16).astype(F32)
    row_lhs[...] = jnp.concatenate([row_high, row_high, row_map - row_high], axis=1).astype(BF16)
    col_map = col_buf[...]
    none = jnp.zeros_like(col_map)
    col_block = jnp.concatenate(
        [jnp.concatenate([col_map, none], axis=1), jnp.concatenate([none, col_map], axis=1)], axis=0
    )
    col_high, col_low = split(col_block)
    col_rhs[...] = jnp.concatenate(
        [
            jnp.concatenate([col_high, col_high], axis=1),
            jnp.concatenate([col_low, jnp.zeros_like(col_low)], axis=1),
        ],
        axis=0,
    )

    @pl.when(coef_self)
    def _():
        pltpu.make_async_copy(coefs.at[pl.ds(0, 7)], coefs.at[pl.ds(0, 7)], coef_got.at[0]).wait()

    @pl.when(jnp.logical_not(coef_self))
    def _():
        pltpu.make_async_copy(coefs, coefs, coef_got.at[0]).wait()

    part[0:3] = jnp.zeros((3, 64, 128), F32)
    part[3] = jnp.ones((64, 128), F32)

    @pl.loop(0, 8)
    def _(j):
        waited = got.at[j, pl.ds(0, 480)]
        pltpu.make_async_copy(waited, waited, got_sem.at[j]).wait()
        for pair in range(4):
            both = jnp.concatenate(
                [got[j, pl.ds(2 * pair + k, 64, stride=8), :] for k in range(2)], axis=1
            )
            high, low = split(both)
            rows = jnp.dot(
                row_lhs[...], jnp.concatenate([high, low, high], axis=0), preferred_element_type=F32
            )
            for k in range(2):
                high, low = split(rows[:, 128 * k : 128 * k + 128])
                at = pl.ds((2 * pair + k) * 64, 64)
                second[at, 0:128] = high
                second[at, 128:256] = low
        wide = dot_nt(second[...], col_rhs[...])
        samples[...] = wide[:, 0:128] + wide[:, 128:256]
        coef = coefs[j]

        @pl.loop(0, 2)
        def _(block):
            at = pl.multiple_of(block * 32, 32)
            rows = pl.ds(at, 32)
            live = entry_buf[rows, :] <= 8 * x + j
            red, green, blue, through = part[0, rows], part[1, rows], part[2, rows], part[3, rows]
            for s in range(8):
                value = samples[pl.ds(at + 64 * s, 32), :]
                tau = STEP_LENGTH * softplus(coef[6:7] * value + coef[7:8])
                kept = jnp.exp(-jnp.where(live, tau, 0.0))
                weight = through * (1.0 - kept)
                through = through * kept
                red = red + weight * softplus(coef[0:1] * value + coef[3:4])
                green = green + weight * softplus(coef[1:2] * value + coef[4:5])
                blue = blue + weight * softplus(coef[2:3] * value + coef[5:6])
            part[0, rows], part[1, rows], part[2, rows], part[3, rows] = red, green, blue, through

    def final_copy(i):
        return remote(
            part.at[:, pl.ds(16 * i, 16)], finals.at[x], fin_send.at[i], fin_got.at[0],
            device(view_zh, view_core, zh, out_y, i),
        )

    for i in range(4):
        final_copy(i).start()
    pltpu.make_async_copy(finals, finals, fin_got.at[0]).wait()
    total = finals[3, 0:3]
    for q in (2, 1, 0):
        total = finals[q, 0:3] + finals[q, 3:4] * total
    out[0] = total

    for i in range(4):
        final_copy(i).wait_send()
    drained = sent.at[pl.ds(0, 15)]
    pltpu.make_async_copy(drained, drained, send_sem.at[0]).wait()

    @pl.when(mine != 0)
    def _():
        for i, (src, dst) in enumerate(maps):
            remote(src, dst, map_send.at[i], map_got.at[i], to_device).wait_send()

    @pl.when(coef_self)
    def _():
        pltpu.make_async_copy(coefs.at[pl.ds(0, 7)], coefs.at[pl.ds(0, 7)], coef_send.at[0]).wait()

    @pl.when(jnp.logical_not(coef_self))
    def _():
        pltpu.make_async_copy(coefs, coefs, coef_send.at[0]).wait()


def render(volume, step_weights, row_interp, col_interp, tf_table, materials, entry):
    vmem = pl.BlockSpec(memory_space=pltpu.VMEM)
    anywhere = pl.BlockSpec(memory_space=pl.ANY)
    smem = pl.BlockSpec(memory_space=pltpu.SMEM)
    dma = pltpu.SemaphoreType.DMA
    return pl.pallas_call(
        kernel,
        name="render",
        out_shape=jax.ShapeDtypeStruct((1, 3, 16, 128), F32),
        in_specs=[anywhere, vmem, anywhere, anywhere, vmem, smem, anywhere],
        out_specs=vmem,
        scratch_shapes=[
            pltpu.VMEM((4, 4, 4, 128, 128), F32),
            pltpu.VMEM((16, 8, 32, 128), F32),
            pltpu.VMEM((8, 512, 128), F32),
            pltpu.VMEM((4, 8, 64), F32),
            pltpu.VMEM((64, 64), F32),
            pltpu.VMEM((64, 64), F32),
            pltpu.VMEM((64, 128), jnp.int32),
            pltpu.VMEM((2, 8, 128), F32),
            pltpu.VMEM((8, 8, 128), F32),
            pltpu.VMEM((64, 192), BF16),
            pltpu.VMEM((256, 256), BF16),
            pltpu.VMEM((512, 256), BF16),
            pltpu.VMEM((512, 128), F32),
            pltpu.VMEM((4, 64, 128), F32),
            pltpu.VMEM((4, 4, 16, 128), F32),
            dma((4, 4)), dma((1,)), dma((8,)), dma((4,)), dma((4,)), dma((3,)), dma((3,)),
            dma((1,)), dma((1,)), dma((4,)), dma((1,)),
        ],
        compiler_params=pltpu.CompilerParams(
            collective_id=0, has_side_effects=True, vmem_limit_bytes=60 * 1024 * 1024
        ),
    )(volume, step_weights, row_interp, col_interp, tf_table, materials, entry)


def solution(mesh):
    torus = Mesh(mesh.devices.reshape(2, 2, 2, 4, 4), AXES)
    return jax.shard_map(
        render,
        mesh=torus,
        in_specs=(
            P(AXES, None, None),
            P(VIEW, None, None),
            P(VIEW, None, None),
            P(VIEW, None, None),
            P(),
            P(None, None, DEPTH),
            P(VIEW, None, None),
        ),
        out_specs=P(VIEW, None, DEPTH, None),
        check_vma=False,
    )
```

```python
import jax
import jax.numpy as jnp
from jax import lax
from jax.experimental import pallas as pl
from jax.experimental.pallas import tpu as pltpu
from jax.sharding import Mesh
from jax.sharding import PartitionSpec as P

AXES = ("zh", "core", "zl", "y", "x")
VIEW = ("zh", "core")
DEPTH = ("zl", "y", "x")
MESH = pl.DeviceIdType.MESH
STEP_LENGTH = 2.0 / 256.0
LOG2E = 1.4426950408889634
LN2 = 0.6931471805599453
BF16 = jnp.bfloat16
F32 = jnp.float32


def split(value):
    high = value.astype(BF16)
    low = (value - high.astype(F32)).astype(BF16)
    return high, low


def dot_nt(lhs, rhs):
    return lax.dot_general(lhs, rhs, (((1,), (1,)), ((), ())), preferred_element_type=F32)


def softplus2(v):
    power = jnp.exp2(jnp.minimum(v, 64.0))
    grown = 1.0 + power
    return jnp.maximum(v, jnp.log2(grown) + LOG2E * (power - (grown - 1.0)))


def step_block(weights):
    twice = jnp.concatenate([weights, weights], axis=1)
    lane = lax.broadcasted_iota(jnp.int32, twice.shape, 1)
    block = jnp.concatenate(
        [jnp.where(lane < 64, twice, 0.0), jnp.where(lane >= 64, twice, 0.0)], axis=0
    )
    high = block.astype(BF16).astype(F32)
    return high, block - high


def step_lhs(weights):
    parts = [step_block(one) for one in weights]
    high = jnp.concatenate([part[0] for part in parts], axis=0)
    low = jnp.concatenate([part[1] for part in parts], axis=0)
    top = jnp.concatenate([high, high], axis=1)
    bottom = jnp.concatenate([low, jnp.zeros_like(low)], axis=1)
    return jnp.concatenate([top, bottom], axis=0).astype(BF16)


ROUNDS = ((0, 2), (2, 2), (4, 2), (6, 1), (7, 1))


def kernel(
    vol, step_map, rows_map, cols_map, table_in, mats_in, entry, out,
    cells, sent, got, weights, table, mats, row_buf, col_buf, entry_buf, coef_own, coef_relay, coefs,
    row_lhs, col_rhs, second, samples, part, finals,
    cell_sem, small_sem, send_sem, got_sem, w_send, w_got, map_send, map_got,
    coef_send, coef_got, pair_send, pair_got, fin_send, fin_got,
):
    zh, core, zl = lax.axis_index("zh"), lax.axis_index("core"), lax.axis_index("zl")
    y, x = lax.axis_index("y"), lax.axis_index("x")

    def cell_copy(rho, q):
        return pltpu.make_async_copy(
            vol.at[:, :, pl.ds(512 * q + 128 * rho, 128)], cells.at[rho, q], cell_sem.at[rho, q]
        )

    small = [
        pltpu.make_async_copy(step_map.at[0], weights.at[0], small_sem.at[0]),
        pltpu.make_async_copy(mats_in, mats, small_sem.at[1]),
        pltpu.make_async_copy(table_in, table, small_sem.at[2]),
    ]
    for copy in small:
        copy.start()
    for rho in range(4):
        for q in range(4):
            cell_copy(rho, q).start()

    place = y * 4 + x
    shift = lax.rem(y - 2 * core - zl + 8, 4)
    mine = lax.rem(2 + 3 * shift, 4)
    view_zh, view_core = lax.rem(zh + mine // 2, 2), lax.rem(core + lax.rem(mine, 2), 2)
    out_y = 2 * core + zl

    def device(zh_=zh, core_=core, zl_=zl, y_=y, x_=x):
        return {"zh": zh_, "core": core_, "zl": zl_, "y": y_, "x": x_}

    def remote(src, dst, send, recv, where):
        return pltpu.make_async_remote_copy(
            src_ref=src, dst_ref=dst, send_sem=send, recv_sem=recv,
            device_id=where, device_id_type=MESH,
        )

    def view_peer(xor):
        return device(zh_=lax.rem(zh + xor // 2, 2), core_=lax.rem(core + xor % 2, 2))

    def take(ref, sem):
        pltpu.make_async_copy(ref, ref, sem).wait()

    brick_slot = lax.rem(y, 2) * 4 + x
    coef_self = lax.rem(x, 2) == y // 2
    barrier = pltpu.get_barrier_semaphore()

    def greet(where):
        pl.semaphore_signal(barrier, inc=1, device_id=where, device_id_type=MESH)

    with jax.named_scope("greet"):
        for xor in (1, 2, 3):
            greet(view_peer(xor))
        for offset in range(15, 0, -1):
            greet(device(y_=lax.rem(y + offset // 4, 4), x_=lax.rem(x + offset % 4, 4)))
        greet(device(zl_=1 - zl))

    def contract(lhs, rho, q, first_view, count):
        high, low = split(cells[rho, q].reshape(512, 128))
        wide = dot_nt(lhs, jnp.concatenate([high, low], axis=1))
        wide = wide[: 16 * count] + wide[16 * count :]
        for k in range(count):
            for pair in range(2):
                for z in range(4):
                    row = 16 * k + 8 * pair
                    sent[(first_view + k) * 4 + q, 2 * rho + pair, pl.ds(8 * z, 8), :] = wide[
                        row : row + 8, 128 * z : 128 * z + 128
                    ]

    def plane_copy(xor, column, first, count, sem):
        peer_y = lax.rem((2 + 3 * xor) % 4 + 2 * core + zl, 4)
        copy = remote(
            sent.at[4 * xor + column, pl.ds(first, count)],
            got.at[pl.ds(first, count), pl.ds(pl.multiple_of(32 * place, 32), 32)],
            send_sem.at[sem], got_sem.at[sem], device(y_=peer_y, x_=column),
        )
        pl.when(jnp.logical_not((mine == xor) & (x == column)))(copy.start)

    def send_round(number, columns=range(4)):
        for xor in range(4):
            for column in columns:
                plane_copy(xor, column, *ROUNDS[number], number)

    def sent_round(number):
        first, count = ROUNDS[number]
        take(sent.at[pl.ds(0, 15), pl.ds(first, count)], send_sem.at[number])

    def send_coefs(plane, source):
        column = plane * 2 + y // 2
        for row in range(4):
            here = (row == y) & (column == x)
            copy = remote(
                source, coefs.at[brick_slot], coef_send.at[0], coef_got.at[0],
                device(y_=row, x_=column),
            )
            pl.when(jnp.logical_not(here))(copy.start)

            @pl.when(here)
            def _():
                coefs[brick_slot] = source[...]

    partner_copy = remote(
        coef_own.at[1 - zl], coef_relay, pair_send.at[0], pair_got.at[0], device(zl_=1 - zl)
    )
    w_copies = [
        remote(weights.at[0], weights.at[xor], w_send.at[xor], w_got.at[xor], view_peer(xor))
        for xor in (1, 2, 3)
    ]
    with jax.named_scope("small"):
        small[0].wait()
    with jax.named_scope("meet"):
        pl.semaphore_wait(barrier, 19)
    for copy in w_copies:
        copy.start()
    with jax.named_scope("classes"):
        for copy in small[1:]:
            copy.wait()
        lane = lax.broadcasted_iota(jnp.int32, (8, 128), 1)
        sublane = lax.broadcasted_iota(jnp.int32, (8, 128), 0)
        for k in range(2):
            tile = 2 * (2 * zh + core) + k
            wanted = jnp.where(lane < 64, mats[0, 0, tile], mats[1, 0, tile])
            onehot = (sublane == wanted).astype(F32)
            coef_own[k] = lax.dot_general(
                table[...], onehot, (((0,), (0,)), ((), ())),
                precision=lax.Precision.HIGHEST, preferred_element_type=F32,
            )
        partner_copy.start()
        send_coefs(zl, coef_own.at[zl])
    own_lhs = step_lhs([weights[0]])
    for rho in range(4):
        with jax.named_scope("wait_cells"):
            for q in range(4):
                cell_copy(rho, q).wait()
        with jax.named_scope("own_view"):
            for q in range(4):
                contract(own_lhs, rho, q, 0, 1)
    to_xor = jnp.where(lax.rem(shift, 2) == 1, lax.rem(2 + 3 * (shift + 2), 4), mine)
    to_zh, to_core = lax.rem(zh + to_xor // 2, 2), lax.rem(core + lax.rem(to_xor, 2), 2)
    to_rows = pl.multiple_of((2 * (2 * to_zh + to_core) + zl) * 64, 64)
    to_device = device(zh_=to_zh, core_=to_core)
    maps = (
        (rows_map.at[0], row_buf),
        (cols_map.at[0], col_buf),
        (entry.at[0, pl.ds(to_rows, 64)], entry_buf),
    )

    with jax.named_scope("wait_weights"):
        for copy in w_copies:
            copy.wait()
    with jax.named_scope("relay"):
        partner_copy.wait()
        send_coefs(1 - zl, coef_relay)
    lhs = step_lhs([weights[xor] for xor in (1, 2, 3)])
    for rho in range(4):
        with jax.named_scope("contract"):
            for q in range(4):
                contract(lhs, rho, q, 1, 3)
                if rho == 0:
                    send_round(0, (q,))
        if rho > 0:
            with jax.named_scope("send_round"):
                for number, (first, _) in enumerate(ROUNDS):
                    if first // 2 == rho:
                        send_round(number)

    @pl.when(mine == 0)
    def _():
        for i, (src, dst) in enumerate(maps):
            pltpu.make_async_copy(src, dst, map_got.at[i]).start()

    @pl.when(mine != 0)
    def _():
        for i, (src, dst) in enumerate(maps):
            remote(src, dst, map_send.at[i], map_got.at[i], to_device).start()

    own_slot = 4 * mine + x

    @pl.loop(0, 8)
    def _(j):
        got[j, pl.ds(pl.multiple_of(32 * place, 32), 32), :] = sent[own_slot, j]

    with jax.named_scope("wait_maps"):
        for i, (src, dst) in enumerate(maps):
            pltpu.make_async_copy(src, dst, map_got.at[i]).wait()

    row_map = row_buf[...]
    row_high = row_map.astype(BF16).astype(F32)
    row_lhs[...] = jnp.concatenate([row_high, row_high, row_map - row_high], axis=1).astype(BF16)
    col_map = col_buf[...]
    none = jnp.zeros_like(col_map)
    col_block = jnp.concatenate(
        [jnp.concatenate([col_map, none], axis=1), jnp.concatenate([none, col_map], axis=1)], axis=0
    )
    col_high, col_low = split(col_block)
    col_rhs[...] = jnp.concatenate(
        [
            jnp.concatenate([col_high, col_high], axis=1),
            jnp.concatenate([col_low, jnp.zeros_like(col_low)], axis=1),
        ],
        axis=0,
    )

    def coef_done(sem):
        pl.when(coef_self)(lambda: take(coefs.at[pl.ds(0, 7)], sem))
        pl.when(jnp.logical_not(coef_self))(lambda: take(coefs, sem))

    with jax.named_scope("wait_classes"):
        coef_done(coef_got.at[0])

    part[0:3] = jnp.zeros((3, 64, 128), F32)
    part[3] = jnp.ones((64, 128), F32)

    def render_brick(j):
        for pair in range(4):
            both = jnp.concatenate(
                [got[j, pl.ds(2 * pair + k, 64, stride=8), :] for k in range(2)], axis=1
            )
            high, low = split(both)
            rows = jnp.dot(
                row_lhs[...], jnp.concatenate([high, low, high], axis=0), preferred_element_type=F32
            )
            for k in range(2):
                high, low = split(rows[:, 128 * k : 128 * k + 128])
                at = pl.ds((2 * pair + k) * 64, 64)
                second[at, 0:128] = high
                second[at, 128:256] = low
        wide = dot_nt(second[...], col_rhs[...])
        samples[...] = wide[:, 0:128] + wide[:, 128:256]
        coef = LOG2E * coefs[j]

        @pl.loop(0, 2)
        def _(block):
            at = pl.multiple_of(block * 32, 32)
            rows = pl.ds(at, 32)
            opacity = jnp.where(entry_buf[rows, :] <= 8 * x + j, -STEP_LENGTH, 0.0)
            red, green, blue, through = part[0, rows], part[1, rows], part[2, rows], part[3, rows]
            for s in range(8):
                value = samples[pl.ds(at + 64 * s, 32), :]
                after = through * jnp.exp2(opacity * softplus2(coef[6:7] * value + coef[7:8]))
                weight = through - after
                through = after
                red = red + weight * softplus2(coef[0:1] * value + coef[3:4])
                green = green + weight * softplus2(coef[1:2] * value + coef[4:5])
                blue = blue + weight * softplus2(coef[2:3] * value + coef[5:6])
            part[0, rows], part[1, rows], part[2, rows], part[3, rows] = red, green, blue, through

    for number, (first, count) in enumerate(ROUNDS):
        with jax.named_scope("wait_brick"):
            take(got.at[pl.ds(first, count), pl.ds(0, 480)], got_sem.at[number])
        with jax.named_scope("bricks"):
            pl.loop(first, first + count)(render_brick)

    def final_copy(i):
        return remote(
            part.at[:, pl.ds(16 * i, 16)], finals.at[x], fin_send.at[i], fin_got.at[0],
            device(view_zh, view_core, zh, out_y, i),
        )

    for i in range(4):
        final_copy(i).start()
    with jax.named_scope("wait_finals"):
        take(finals, fin_got.at[0])
    total = finals[3, 0:3]
    for q in (2, 1, 0):
        total = finals[q, 0:3] + finals[q, 3:4] * total
    out[0] = LN2 * total

    for i in range(4):
        final_copy(i).wait_send()
    with jax.named_scope("drain"):
        for number in range(len(ROUNDS)):
            sent_round(number)

    @pl.when(mine != 0)
    def _():
        for i, (src, dst) in enumerate(maps):
            remote(src, dst, map_send.at[i], map_got.at[i], to_device).wait_send()

    coef_done(coef_send.at[0])


def render(volume, step_weights, row_interp, col_interp, tf_table, materials, entry):
    vmem = pl.BlockSpec(memory_space=pltpu.VMEM)
    anywhere = pl.BlockSpec(memory_space=pl.ANY)
    dma = pltpu.SemaphoreType.DMA
    return pl.pallas_call(
        kernel,
        name="render",
        out_shape=pltpu.VMEM((1, 3, 16, 128), F32),
        in_specs=[anywhere] * 7,
        out_specs=vmem,
        scratch_shapes=[
            pltpu.VMEM((4, 4, 4, 128, 128), F32),
            pltpu.VMEM((16, 8, 32, 128), F32),
            pltpu.VMEM((8, 512, 128), F32),
            pltpu.VMEM((4, 8, 64), F32),
            pltpu.VMEM((8, 8), F32),
            pltpu.SMEM((2, 1, 8), jnp.int32),
            pltpu.VMEM((64, 64), F32),
            pltpu.VMEM((64, 64), F32),
            pltpu.VMEM((64, 128), jnp.int32),
            pltpu.VMEM((2, 8, 128), F32),
            pltpu.VMEM((8, 128), F32),
            pltpu.VMEM((8, 8, 128), F32),
            pltpu.VMEM((64, 192), BF16),
            pltpu.VMEM((256, 256), BF16),
            pltpu.VMEM((512, 256), BF16),
            pltpu.VMEM((512, 128), F32),
            pltpu.VMEM((4, 64, 128), F32),
            pltpu.VMEM((4, 4, 16, 128), F32),
            dma((4, 4)), dma((3,)), dma((5,)), dma((5,)), dma((4,)), dma((4,)), dma((3,)), dma((3,)),
            dma((1,)), dma((1,)), dma((1,)), dma((1,)), dma((4,)), dma((1,)),
        ],
        compiler_params=pltpu.CompilerParams(
            collective_id=0, has_side_effects=True, vmem_limit_bytes=60 * 1024 * 1024
        ),
    )(
        volume, step_weights, row_interp, col_interp, tf_table, materials.transpose(1, 2, 0), entry
    )


def solution(mesh):
    torus = Mesh(mesh.devices.reshape(2, 2, 2, 4, 4), AXES)
    return jax.shard_map(
        render,
        mesh=torus,
        in_specs=(
            P(AXES, None, None),
            P(VIEW, None, None),
            P(VIEW, None, None),
            P(VIEW, None, None),
            P(),
            P(None, None, DEPTH),
            P(VIEW, None, None),
        ),
        out_specs=P(VIEW, None, DEPTH, None),
        check_vma=False,
    )
```

```python
import jax
import jax.numpy as jnp
from jax import lax
from jax.experimental import pallas as pl
from jax.experimental.pallas import tpu as pltpu
from jax.sharding import Mesh
from jax.sharding import PartitionSpec as P

AXES = ("zh", "core", "zl", "y", "x")
VIEW = ("zh", "core")
DEPTH = ("zl", "y", "x")
MESH = pl.DeviceIdType.MESH
STEP_LENGTH = 2.0 / 256.0
LOG2E = 1.4426950408889634
LN2 = 0.6931471805599453
BF16 = jnp.bfloat16
F32 = jnp.float32


def split(value):
    high = value.astype(BF16)
    low = (value - high.astype(F32)).astype(BF16)
    return high, low


def dot_nt(lhs, rhs):
    return lax.dot_general(lhs, rhs, (((1,), (1,)), ((), ())), preferred_element_type=F32)


def softplus2(v):
    power = jnp.exp2(jnp.minimum(v, 64.0))
    grown = 1.0 + power
    return jnp.maximum(v, jnp.log2(grown) + LOG2E * (power - (grown - 1.0)))


def step_block(weights):
    twice = jnp.concatenate([weights, weights], axis=1)
    lane = lax.broadcasted_iota(jnp.int32, twice.shape, 1)
    block = jnp.concatenate(
        [jnp.where(lane < 64, twice, 0.0), jnp.where(lane >= 64, twice, 0.0)], axis=0
    )
    high = block.astype(BF16).astype(F32)
    return high, block - high


def step_lhs(weights):
    parts = [step_block(one) for one in weights]
    high = jnp.concatenate([part[0] for part in parts], axis=0)
    low = jnp.concatenate([part[1] for part in parts], axis=0)
    top = jnp.concatenate([high, high], axis=1)
    bottom = jnp.concatenate([low, jnp.zeros_like(low)], axis=1)
    return jnp.concatenate([top, bottom], axis=0).astype(BF16)


ROUNDS = ((0, 2), (2, 2), (4, 2), (6, 1), (7, 1))


def kernel(
    vol, step_map, rows_map, cols_map, table_in, mats_in, entry, out,
    cells, sent, got, weights, table, mats, row_buf, col_buf, entry_buf, coef_own, coef_relay, coefs,
    row_lhs, col_rhs, second, samples, part, finals,
    cell_sem, small_sem, send_sem, got_sem, w_send, w_got, map_send, map_got,
    coef_send, coef_got, pair_send, pair_got, fin_send, fin_got, row_ready, plane_ready,
):
    zh, core, zl = lax.axis_index("zh"), lax.axis_index("core"), lax.axis_index("zl")
    y, x = lax.axis_index("y"), lax.axis_index("x")

    def cell_copy(rho, q):
        return pltpu.make_async_copy(
            vol.at[:, :, pl.ds(512 * q + 128 * rho, 128)], cells.at[rho, q], cell_sem.at[rho, q]
        )

    small = [
        pltpu.make_async_copy(step_map.at[0], weights.at[0], small_sem.at[0]),
        pltpu.make_async_copy(mats_in, mats, small_sem.at[1]),
        pltpu.make_async_copy(table_in, table, small_sem.at[2]),
    ]
    for copy in small:
        copy.start()

    place = y * 4 + x
    shift = lax.rem(y - 2 * core - zl + 8, 4)
    mine = lax.rem(2 + 3 * shift, 4)
    view_zh, view_core = lax.rem(zh + mine // 2, 2), lax.rem(core + lax.rem(mine, 2), 2)
    out_y = 2 * core + zl

    def device(zh_=zh, core_=core, zl_=zl, y_=y, x_=x):
        return {"zh": zh_, "core": core_, "zl": zl_, "y": y_, "x": x_}

    def remote(src, dst, send, recv, where):
        return pltpu.make_async_remote_copy(
            src_ref=src, dst_ref=dst, send_sem=send, recv_sem=recv,
            device_id=where, device_id_type=MESH,
        )

    def view_peer(xor):
        return device(zh_=lax.rem(zh + xor // 2, 2), core_=lax.rem(core + xor % 2, 2))

    def take(ref, sem):
        pltpu.make_async_copy(ref, ref, sem).wait()

    brick_slot = lax.rem(y, 2) * 4 + x
    coef_self = lax.rem(x, 2) == y // 2
    barrier = pltpu.get_barrier_semaphore()

    def greet(where):
        pl.semaphore_signal(barrier, inc=1, device_id=where, device_id_type=MESH)

    rows = [device(x_=lax.rem(x + i, 4)) for i in (2, 1, 3)]
    columns = [device(y_=lax.rem(y + i, 4)) for i in (2, 1, 3)]
    pair = device(zl_=1 - zl)
    with jax.named_scope("greet"):
        for peer in [view_peer(2), view_peer(3)] + rows + columns + [pair, view_peer(1)]:
            greet(peer)
    for rho in range(4):
        for q in range(4):
            cell_copy(rho, q).start()

    def contract(lhs, rho, q, first_view, count):
        high, low = split(cells[rho, q].reshape(512, 128))
        wide = dot_nt(lhs, jnp.concatenate([high, low], axis=1))
        wide = wide[: 16 * count] + wide[16 * count :]
        for k in range(count):
            for pair in range(2):
                for z in range(4):
                    row = 16 * k + 8 * pair
                    sent[(first_view + k) * 4 + q, 2 * rho + pair, pl.ds(8 * z, 8), :] = wide[
                        row : row + 8, 128 * z : 128 * z + 128
                    ]

    def plane_copy(xor, column, first, count, sem):
        peer_y = lax.rem((2 + 3 * xor) % 4 + 2 * core + zl, 4)
        copy = remote(
            sent.at[4 * xor + column, pl.ds(first, count)],
            got.at[pl.ds(first, count), pl.ds(pl.multiple_of(32 * place, 32), 32)],
            send_sem.at[sem], got_sem.at[sem], device(y_=peer_y, x_=column),
        )
        pl.when(jnp.logical_not((mine == xor) & (x == column)))(copy.start)

    def send_round(number, columns=range(4)):
        for xor in range(4):
            for column in columns:
                plane_copy(xor, column, *ROUNDS[number], number)

    def sent_round(number):
        first, count = ROUNDS[number]
        take(sent.at[pl.ds(0, 15), pl.ds(first, count)], send_sem.at[number])

    def send_coefs(plane, source):
        column = plane * 2 + y // 2
        for row in range(4):
            here = (row == y) & (column == x)
            copy = remote(
                source, coefs.at[brick_slot], coef_send.at[0], coef_got.at[0],
                device(y_=row, x_=column),
            )
            pl.when(jnp.logical_not(here))(copy.start)

            @pl.when(here)
            def _():
                coefs[brick_slot] = source[...]

    partner_copy = remote(
        coef_own.at[1 - zl], coef_relay, pair_send.at[0], pair_got.at[0], pair
    )
    w_copies = [
        remote(weights.at[0], weights.at[xor], w_send.at[xor], w_got.at[xor], view_peer(xor))
        for xor in (1, 2, 3)
    ]
    with jax.named_scope("small"):
        small[0].wait()
    with jax.named_scope("meet"):
        pl.semaphore_wait(barrier, 10)
    for copy in w_copies:
        copy.start()
    for peer in columns:
        pl.semaphore_signal(row_ready, inc=1, device_id=peer, device_id_type=MESH)
    with jax.named_scope("classes"):
        for copy in small[1:]:
            copy.wait()
        lane = lax.broadcasted_iota(jnp.int32, (8, 128), 1)
        sublane = lax.broadcasted_iota(jnp.int32, (8, 128), 0)
        for k in range(2):
            tile = 2 * (2 * zh + core) + k
            wanted = jnp.where(lane < 64, mats[0, 0, tile], mats[1, 0, tile])
            onehot = (sublane == wanted).astype(F32)
            coef_own[k] = lax.dot_general(
                table[...], onehot, (((0,), (0,)), ((), ())),
                precision=lax.Precision.HIGHEST, preferred_element_type=F32,
            )
        partner_copy.start()
    own_lhs = step_lhs([weights[0]])

    def own_view(rho):
        with jax.named_scope("wait_cells"):
            for q in range(4):
                cell_copy(rho, q).wait()
        with jax.named_scope("own_view"):
            for q in range(4):
                contract(own_lhs, rho, q, 0, 1)

    own_view(0)
    own_view(1)
    with jax.named_scope("plane"):
        pl.semaphore_wait(row_ready, 3)
    pl.semaphore_signal(plane_ready, inc=1, device_id=pair, device_id_type=MESH)
    send_coefs(zl, coef_own.at[zl])
    own_view(2)
    own_view(3)
    to_xor = jnp.where(lax.rem(shift, 2) == 1, lax.rem(2 + 3 * (shift + 2), 4), mine)
    to_zh, to_core = lax.rem(zh + to_xor // 2, 2), lax.rem(core + lax.rem(to_xor, 2), 2)
    to_rows = pl.multiple_of((2 * (2 * to_zh + to_core) + zl) * 64, 64)
    to_device = device(zh_=to_zh, core_=to_core)
    maps = (
        (rows_map.at[0], row_buf),
        (cols_map.at[0], col_buf),
        (entry.at[0, pl.ds(to_rows, 64)], entry_buf),
    )

    with jax.named_scope("wait_weights"):
        for copy in w_copies:
            copy.wait()
    lhs = step_lhs([weights[xor] for xor in (1, 2, 3)])
    for rho in range(4):
        with jax.named_scope("contract"):
            for i in range(4):
                q = lax.rem(x + i, 4) if rho == 0 else i
                contract(lhs, rho, q, 1, 3)
                if rho == 0:
                    send_round(0, (q,))
        if rho == 0:
            with jax.named_scope("relay"):
                partner_copy.wait()
                send_coefs(1 - zl, coef_relay)
        if rho > 0:
            with jax.named_scope("send_round"):
                for number, (first, _) in enumerate(ROUNDS):
                    if first // 2 == rho:
                        send_round(number)

    pl.semaphore_wait(plane_ready, 1)

    @pl.when(mine == 0)
    def _():
        for i, (src, dst) in enumerate(maps):
            pltpu.make_async_copy(src, dst, map_got.at[i]).start()

    @pl.when(mine != 0)
    def _():
        for i, (src, dst) in enumerate(maps):
            remote(src, dst, map_send.at[i], map_got.at[i], to_device).start()

    own_slot = 4 * mine + x

    @pl.loop(0, 8)
    def _(j):
        got[j, pl.ds(pl.multiple_of(32 * place, 32), 32), :] = sent[own_slot, j]

    with jax.named_scope("wait_maps"):
        for i, (src, dst) in enumerate(maps):
            pltpu.make_async_copy(src, dst, map_got.at[i]).wait()

    row_map = row_buf[...]
    row_high = row_map.astype(BF16).astype(F32)
    row_lhs[...] = jnp.concatenate([row_high, row_high, row_map - row_high], axis=1).astype(BF16)
    col_map = col_buf[...]
    none = jnp.zeros_like(col_map)
    col_block = jnp.concatenate(
        [jnp.concatenate([col_map, none], axis=1), jnp.concatenate([none, col_map], axis=1)], axis=0
    )
    col_high, col_low = split(col_block)
    col_rhs[...] = jnp.concatenate(
        [
            jnp.concatenate([col_high, col_high], axis=1),
            jnp.concatenate([col_low, jnp.zeros_like(col_low)], axis=1),
        ],
        axis=0,
    )

    def coef_done(sem):
        pl.when(coef_self)(lambda: take(coefs.at[pl.ds(0, 7)], sem))
        pl.when(jnp.logical_not(coef_self))(lambda: take(coefs, sem))

    with jax.named_scope("wait_classes"):
        coef_done(coef_got.at[0])

    part[0:3] = jnp.zeros((3, 64, 128), F32)
    part[3] = jnp.ones((64, 128), F32)

    def sample_brick(j):
        for pair in range(4):
            both = jnp.concatenate(
                [got[j, pl.ds(2 * pair + k, 64, stride=8), :] for k in range(2)], axis=1
            )
            high, low = split(both)
            rows = jnp.dot(
                row_lhs[...], jnp.concatenate([high, low, high], axis=0), preferred_element_type=F32
            )
            for k in range(2):
                high, low = split(rows[:, 128 * k : 128 * k + 128])
                at = pl.ds((2 * pair + k) * 64, 64)
                second[at, 0:128] = high
                second[at, 128:256] = low
        wide = dot_nt(second[...], col_rhs[...])
        samples[...] = wide[:, 0:128] + wide[:, 128:256]

    def shade(j, at):
        coef = LOG2E * coefs[j]
        rows = pl.ds(at, 32)
        opacity = jnp.where(entry_buf[rows, :] <= 8 * x + j, -STEP_LENGTH, 0.0)
        red, green, blue, through = part[0, rows], part[1, rows], part[2, rows], part[3, rows]
        for s in range(8):
            value = samples[pl.ds(at + 64 * s, 32), :]
            after = through * jnp.exp2(opacity * softplus2(coef[6:7] * value + coef[7:8]))
            weight = through - after
            through = after
            red = red + weight * softplus2(coef[0:1] * value + coef[3:4])
            green = green + weight * softplus2(coef[1:2] * value + coef[4:5])
            blue = blue + weight * softplus2(coef[2:3] * value + coef[5:6])
        part[0, rows], part[1, rows], part[2, rows], part[3, rows] = red, green, blue, through

    def final_copy(i):
        return remote(
            part.at[:, pl.ds(16 * i, 16)], finals.at[x], fin_send.at[i], fin_got.at[0],
            device(view_zh, view_core, zh, out_y, i),
        )

    for number, (first, count) in enumerate(ROUNDS):
        with jax.named_scope("wait_brick"):
            take(got.at[pl.ds(first, count), pl.ds(0, 480)], got_sem.at[number])
        with jax.named_scope("bricks"):
            @pl.loop(first, first + count)
            def _(j):
                sample_brick(j)
                if first + count < 8:
                    pl.loop(0, 2)(lambda block: shade(j, pl.multiple_of(block * 32, 32)))
                else:
                    for block in range(2):
                        shade(j, 32 * block)
                        final_copy(2 * block).start()
                        final_copy(2 * block + 1).start()

    with jax.named_scope("wait_finals"):
        take(finals, fin_got.at[0])
    total = finals[3, 0:3]
    for q in (2, 1, 0):
        total = finals[q, 0:3] + finals[q, 3:4] * total
    out[0] = LN2 * total

    for i in range(4):
        final_copy(i).wait_send()
    with jax.named_scope("drain"):
        for number in range(len(ROUNDS)):
            sent_round(number)

    @pl.when(mine != 0)
    def _():
        for i, (src, dst) in enumerate(maps):
            remote(src, dst, map_send.at[i], map_got.at[i], to_device).wait_send()

    coef_done(coef_send.at[0])


def render(volume, step_weights, row_interp, col_interp, tf_table, materials, entry):
    vmem = pl.BlockSpec(memory_space=pltpu.VMEM)
    anywhere = pl.BlockSpec(memory_space=pl.ANY)
    dma = pltpu.SemaphoreType.DMA
    return pl.pallas_call(
        kernel,
        name="render",
        out_shape=pltpu.VMEM((1, 3, 16, 128), F32),
        in_specs=[anywhere] * 7,
        out_specs=vmem,
        scratch_shapes=[
            pltpu.VMEM((4, 4, 4, 128, 128), F32),
            pltpu.VMEM((16, 8, 32, 128), F32),
            pltpu.VMEM((8, 512, 128), F32),
            pltpu.VMEM((4, 8, 64), F32),
            pltpu.VMEM((8, 8), F32),
            pltpu.SMEM((2, 1, 8), jnp.int32),
            pltpu.VMEM((64, 64), F32),
            pltpu.VMEM((64, 64), F32),
            pltpu.VMEM((64, 128), jnp.int32),
            pltpu.VMEM((2, 8, 128), F32),
            pltpu.VMEM((8, 128), F32),
            pltpu.VMEM((8, 8, 128), F32),
            pltpu.VMEM((64, 192), BF16),
            pltpu.VMEM((256, 256), BF16),
            pltpu.VMEM((512, 256), BF16),
            pltpu.VMEM((512, 128), F32),
            pltpu.VMEM((4, 64, 128), F32),
            pltpu.VMEM((4, 4, 16, 128), F32),
            dma((4, 4)), dma((3,)), dma((5,)), dma((5,)), dma((4,)), dma((4,)), dma((3,)), dma((3,)),
            dma((1,)), dma((1,)), dma((1,)), dma((1,)), dma((4,)), dma((1,)),
            pltpu.SemaphoreType.REGULAR, pltpu.SemaphoreType.REGULAR,
        ],
        compiler_params=pltpu.CompilerParams(
            collective_id=0, has_side_effects=True, vmem_limit_bytes=60 * 1024 * 1024
        ),
    )(
        volume, step_weights, row_interp, col_interp, tf_table, materials.transpose(1, 2, 0), entry
    )


def solution(mesh):
    torus = Mesh(mesh.devices.reshape(2, 2, 2, 4, 4), AXES)
    return jax.shard_map(
        render,
        mesh=torus,
        in_specs=(
            P(AXES, None, None),
            P(VIEW, None, None),
            P(VIEW, None, None),
            P(VIEW, None, None),
            P(),
            P(None, None, DEPTH),
            P(VIEW, None, None),
        ),
        out_specs=P(VIEW, None, DEPTH, None),
        check_vma=False,
    )
```

```python
import jax
import jax.numpy as jnp
from jax import lax
from jax.experimental import pallas as pl
from jax.experimental.pallas import tpu as pltpu
from jax.sharding import Mesh
from jax.sharding import PartitionSpec as P

AXES = ("zh", "core", "zl", "y", "x")
VIEW = ("zh", "core")
DEPTH = ("zl", "y", "x")
MESH = pl.DeviceIdType.MESH
STEP_LENGTH = 2.0 / 256.0
LOG2E = 1.4426950408889634
LN2 = 0.6931471805599453
BF16 = jnp.bfloat16
F32 = jnp.float32


def split(value):
    high = value.astype(BF16)
    low = (value - high.astype(F32)).astype(BF16)
    return high, low


def dot_nt(lhs, rhs):
    return lax.dot_general(lhs, rhs, (((1,), (1,)), ((), ())), preferred_element_type=F32)


def softplus2(v):
    power = jnp.exp2(jnp.minimum(v, 64.0))
    grown = 1.0 + power
    return jnp.maximum(v, jnp.log2(grown) + LOG2E * (power - (grown - 1.0)))


def step_block(weights):
    twice = jnp.concatenate([weights, weights], axis=1)
    lane = lax.broadcasted_iota(jnp.int32, twice.shape, 1)
    block = jnp.concatenate(
        [jnp.where(lane < 64, twice, 0.0), jnp.where(lane >= 64, twice, 0.0)], axis=0
    )
    high = block.astype(BF16).astype(F32)
    return high, block - high


def step_lhs(weights):
    parts = [step_block(one) for one in weights]
    high = jnp.concatenate([part[0] for part in parts], axis=0)
    low = jnp.concatenate([part[1] for part in parts], axis=0)
    top = jnp.concatenate([high, high], axis=1)
    bottom = jnp.concatenate([low, jnp.zeros_like(low)], axis=1)
    return jnp.concatenate([top, bottom], axis=0).astype(BF16)


ROUNDS = ((0, 2), (2, 2), (4, 1), (5, 1), (6, 1), (7, 1))


def kernel(
    vol, step_map, rows_map, cols_map, table_in, mats_in, entry, out,
    cells, sent, got, weights, table, mats, row_buf, col_buf, entry_buf, coef_own, coef_relay, coefs,
    row_lhs, col_rhs, second, samples, part, finals,
    cell_sem, small_sem, send_sem, got_sem, w_send, w_got, map_send, map_got,
    coef_send, coef_got, pair_send, pair_got, fin_send, fin_got, row_ready, plane_ready,
):
    zh, core, zl = lax.axis_index("zh"), lax.axis_index("core"), lax.axis_index("zl")
    y, x = lax.axis_index("y"), lax.axis_index("x")

    def cell_copy(rho, q):
        return pltpu.make_async_copy(
            vol.at[:, :, pl.ds(512 * q + 128 * rho, 128)], cells.at[rho, q], cell_sem.at[rho, q]
        )

    small = [
        pltpu.make_async_copy(step_map.at[0], weights.at[0], small_sem.at[0]),
        pltpu.make_async_copy(mats_in, mats, small_sem.at[1]),
        pltpu.make_async_copy(table_in, table, small_sem.at[2]),
    ]
    for copy in small:
        copy.start()

    place = y * 4 + x
    shift = lax.rem(y - 2 * core - zl + 8, 4)
    mine = lax.rem(2 + 3 * shift, 4)
    view_zh, view_core = lax.rem(zh + mine // 2, 2), lax.rem(core + lax.rem(mine, 2), 2)
    out_y = 2 * core + zl

    def device(zh_=zh, core_=core, zl_=zl, y_=y, x_=x):
        return {"zh": zh_, "core": core_, "zl": zl_, "y": y_, "x": x_}

    def remote(src, dst, send, recv, where):
        return pltpu.make_async_remote_copy(
            src_ref=src, dst_ref=dst, send_sem=send, recv_sem=recv,
            device_id=where, device_id_type=MESH,
        )

    def view_peer(xor):
        return device(zh_=lax.rem(zh + xor // 2, 2), core_=lax.rem(core + xor % 2, 2))

    def take(ref, sem):
        pltpu.make_async_copy(ref, ref, sem).wait()

    brick_slot = lax.rem(y, 2) * 4 + x
    coef_self = lax.rem(x, 2) == y // 2
    barrier = pltpu.get_barrier_semaphore()

    def greet(where):
        pl.semaphore_signal(barrier, inc=1, device_id=where, device_id_type=MESH)

    rows = [device(x_=lax.rem(x + i, 4)) for i in (2, 1, 3)]
    columns = [device(y_=lax.rem(y + i, 4)) for i in (2, 1, 3)]
    pair = device(zl_=1 - zl)
    with jax.named_scope("greet"):
        for peer in [view_peer(2), view_peer(3)] + rows + columns + [pair, view_peer(1)]:
            greet(peer)
    for rho in range(4):
        for q in range(4):
            cell_copy(rho, q).start()

    def contract(lhs, rho, q, first_view, count):
        high, low = split(cells[rho, q].reshape(512, 128))
        wide = dot_nt(lhs, jnp.concatenate([high, low], axis=1))
        wide = wide[: 16 * count] + wide[16 * count :]
        for k in range(count):
            for pair in range(2):
                for z in range(4):
                    row = 16 * k + 8 * pair
                    sent[(first_view + k) * 4 + q, 2 * rho + pair, pl.ds(8 * z, 8), :] = wide[
                        row : row + 8, 128 * z : 128 * z + 128
                    ]

    def plane_copy(xor, column, first, count, sem):
        peer_y = lax.rem((2 + 3 * xor) % 4 + 2 * core + zl, 4)
        copy = remote(
            sent.at[4 * xor + column, pl.ds(first, count)],
            got.at[pl.ds(first, count), pl.ds(pl.multiple_of(32 * place, 32), 32)],
            send_sem.at[sem], got_sem.at[sem], device(y_=peer_y, x_=column),
        )
        pl.when(jnp.logical_not((mine == xor) & (x == column)))(copy.start)

    def send_round(number, columns=range(4)):
        for xor in range(4):
            for column in columns:
                plane_copy(xor, column, *ROUNDS[number], number)

    def sent_round(number):
        first, count = ROUNDS[number]
        take(sent.at[pl.ds(0, 15), pl.ds(first, count)], send_sem.at[number])

    def send_coefs(plane, source):
        column = plane * 2 + y // 2
        for row in range(4):
            here = (row == y) & (column == x)
            copy = remote(
                source, coefs.at[brick_slot], coef_send.at[0], coef_got.at[0],
                device(y_=row, x_=column),
            )
            pl.when(jnp.logical_not(here))(copy.start)

            @pl.when(here)
            def _():
                coefs[brick_slot] = source[...]

    partner_copy = remote(
        coef_own.at[1 - zl], coef_relay, pair_send.at[0], pair_got.at[0], pair
    )
    w_copies = [
        remote(weights.at[0], weights.at[xor], w_send.at[xor], w_got.at[xor], view_peer(xor))
        for xor in (1, 2, 3)
    ]
    with jax.named_scope("small"):
        small[0].wait()
    with jax.named_scope("meet"):
        pl.semaphore_wait(barrier, 10)
    for copy in w_copies:
        copy.start()
    for peer in columns:
        pl.semaphore_signal(row_ready, inc=1, device_id=peer, device_id_type=MESH)
    with jax.named_scope("classes"):
        for copy in small[1:]:
            copy.wait()
        lane = lax.broadcasted_iota(jnp.int32, (8, 128), 1)
        sublane = lax.broadcasted_iota(jnp.int32, (8, 128), 0)
        for k in range(2):
            tile = 2 * (2 * zh + core) + k
            wanted = jnp.where(lane < 64, mats[0, 0, tile], mats[1, 0, tile])
            onehot = (sublane == wanted).astype(F32)
            coef_own[k] = lax.dot_general(
                table[...], onehot, (((0,), (0,)), ((), ())),
                precision=lax.Precision.HIGHEST, preferred_element_type=F32,
            )
        partner_copy.start()
    own_lhs = step_lhs([weights[0]])

    def own_view(rho):
        with jax.named_scope("wait_cells"):
            for q in range(4):
                cell_copy(rho, q).wait()
        with jax.named_scope("own_view"):
            for q in range(4):
                contract(own_lhs, rho, q, 0, 1)

    own_view(0)
    own_view(1)
    with jax.named_scope("plane"):
        pl.semaphore_wait(row_ready, 3)
    pl.semaphore_signal(plane_ready, inc=1, device_id=pair, device_id_type=MESH)
    send_coefs(zl, coef_own.at[zl])
    own_view(2)
    own_view(3)
    to_xor = jnp.where(lax.rem(shift, 2) == 1, lax.rem(2 + 3 * (shift + 2), 4), mine)
    to_zh, to_core = lax.rem(zh + to_xor // 2, 2), lax.rem(core + lax.rem(to_xor, 2), 2)
    to_rows = pl.multiple_of((2 * (2 * to_zh + to_core) + zl) * 64, 64)
    to_device = device(zh_=to_zh, core_=to_core)
    maps = (
        (rows_map.at[0], row_buf),
        (cols_map.at[0], col_buf),
        (entry.at[0, pl.ds(to_rows, 64)], entry_buf),
    )

    with jax.named_scope("relay"):
        partner_copy.wait()
        send_coefs(1 - zl, coef_relay)
    with jax.named_scope("wait_weights"):
        for copy in w_copies:
            copy.wait()
    lhs = step_lhs([weights[xor] for xor in (1, 2, 3)])
    for rho in range(4):
        with jax.named_scope("contract"):
            for i in range(4):
                q = lax.rem(x + i, 4) if rho == 0 else i
                contract(lhs, rho, q, 1, 3)
                if rho == 0:
                    send_round(0, (q,))
        if rho > 0:
            with jax.named_scope("send_round"):
                for number, (first, count) in enumerate(ROUNDS):
                    if (first + count - 1) // 2 == rho:
                        send_round(number)

    pl.semaphore_wait(plane_ready, 1)

    @pl.when(mine == 0)
    def _():
        for i, (src, dst) in enumerate(maps):
            pltpu.make_async_copy(src, dst, map_got.at[i]).start()

    @pl.when(mine != 0)
    def _():
        for i, (src, dst) in enumerate(maps):
            remote(src, dst, map_send.at[i], map_got.at[i], to_device).start()

    own_slot = 4 * mine + x

    @pl.loop(0, 8)
    def _(j):
        got[j, pl.ds(pl.multiple_of(32 * place, 32), 32), :] = sent[own_slot, j]

    with jax.named_scope("wait_maps"):
        for i, (src, dst) in enumerate(maps):
            pltpu.make_async_copy(src, dst, map_got.at[i]).wait()

    row_map = row_buf[...]
    row_high = row_map.astype(BF16).astype(F32)
    row_lhs[...] = jnp.concatenate([row_high, row_high, row_map - row_high], axis=1).astype(BF16)
    col_map = col_buf[...]
    none = jnp.zeros_like(col_map)
    col_block = jnp.concatenate(
        [jnp.concatenate([col_map, none], axis=1), jnp.concatenate([none, col_map], axis=1)], axis=0
    )
    col_high, col_low = split(col_block)
    col_rhs[...] = jnp.concatenate(
        [
            jnp.concatenate([col_high, col_high], axis=1),
            jnp.concatenate([col_low, jnp.zeros_like(col_low)], axis=1),
        ],
        axis=0,
    )

    def coef_done(sem):
        pl.when(coef_self)(lambda: take(coefs.at[pl.ds(0, 7)], sem))
        pl.when(jnp.logical_not(coef_self))(lambda: take(coefs, sem))

    with jax.named_scope("wait_classes"):
        coef_done(coef_got.at[0])

    part[0:3] = jnp.zeros((3, 64, 128), F32)
    part[3] = jnp.ones((64, 128), F32)

    def sample_brick(j):
        for pair in range(4):
            both = jnp.concatenate(
                [got[j, pl.ds(2 * pair + k, 64, stride=8), :] for k in range(2)], axis=1
            )
            high, low = split(both)
            rows = jnp.dot(
                row_lhs[...], jnp.concatenate([high, low, high], axis=0), preferred_element_type=F32
            )
            for k in range(2):
                high, low = split(rows[:, 128 * k : 128 * k + 128])
                at = pl.ds((2 * pair + k) * 64, 64)
                second[at, 0:128] = high
                second[at, 128:256] = low
        wide = dot_nt(second[...], col_rhs[...])
        samples[...] = wide[:, 0:128] + wide[:, 128:256]

    def shade(j, at):
        coef = LOG2E * coefs[j]
        rows = pl.ds(at, 32)
        opacity = jnp.where(entry_buf[rows, :] <= 8 * x + j, -STEP_LENGTH, 0.0)
        red, green, blue, through = part[0, rows], part[1, rows], part[2, rows], part[3, rows]
        for s in range(8):
            value = samples[pl.ds(at + 64 * s, 32), :]
            after = through * jnp.exp2(opacity * softplus2(coef[6:7] * value + coef[7:8]))
            weight = through - after
            through = after
            red = red + weight * softplus2(coef[0:1] * value + coef[3:4])
            green = green + weight * softplus2(coef[1:2] * value + coef[4:5])
            blue = blue + weight * softplus2(coef[2:3] * value + coef[5:6])
        part[0, rows], part[1, rows], part[2, rows], part[3, rows] = red, green, blue, through

    def final_copy(i):
        return remote(
            part.at[:, pl.ds(16 * i, 16)], finals.at[x], fin_send.at[i], fin_got.at[0],
            device(view_zh, view_core, zh, out_y, i),
        )

    for number, (first, count) in enumerate(ROUNDS):
        with jax.named_scope("wait_brick"):
            take(got.at[pl.ds(first, count), pl.ds(0, 480)], got_sem.at[number])
        with jax.named_scope("bricks"):
            @pl.loop(first, first + count)
            def _(j):
                sample_brick(j)
                if first + count < 8:
                    pl.loop(0, 2)(lambda block: shade(j, pl.multiple_of(block * 32, 32)))
                else:
                    for block in range(2):
                        shade(j, 32 * block)
                        final_copy(2 * block).start()
                        final_copy(2 * block + 1).start()

    with jax.named_scope("wait_finals"):
        take(finals, fin_got.at[0])
    total = finals[3, 0:3]
    for q in (2, 1, 0):
        total = finals[q, 0:3] + finals[q, 3:4] * total
    out[0] = LN2 * total

    for i in range(4):
        final_copy(i).wait_send()
    with jax.named_scope("drain"):
        for number in range(len(ROUNDS)):
            sent_round(number)

    @pl.when(mine != 0)
    def _():
        for i, (src, dst) in enumerate(maps):
            remote(src, dst, map_send.at[i], map_got.at[i], to_device).wait_send()

    coef_done(coef_send.at[0])


def render(volume, step_weights, row_interp, col_interp, tf_table, materials, entry):
    vmem = pl.BlockSpec(memory_space=pltpu.VMEM)
    anywhere = pl.BlockSpec(memory_space=pl.ANY)
    dma = pltpu.SemaphoreType.DMA
    return pl.pallas_call(
        kernel,
        name="render",
        out_shape=pltpu.VMEM((1, 3, 16, 128), F32),
        in_specs=[anywhere] * 7,
        out_specs=vmem,
        scratch_shapes=[
            pltpu.VMEM((4, 4, 4, 128, 128), F32),
            pltpu.VMEM((16, 8, 32, 128), F32),
            pltpu.VMEM((8, 512, 128), F32),
            pltpu.VMEM((4, 8, 64), F32),
            pltpu.VMEM((8, 8), F32),
            pltpu.SMEM((2, 1, 8), jnp.int32),
            pltpu.VMEM((64, 64), F32),
            pltpu.VMEM((64, 64), F32),
            pltpu.VMEM((64, 128), jnp.int32),
            pltpu.VMEM((2, 8, 128), F32),
            pltpu.VMEM((8, 128), F32),
            pltpu.VMEM((8, 8, 128), F32),
            pltpu.VMEM((64, 192), BF16),
            pltpu.VMEM((256, 256), BF16),
            pltpu.VMEM((512, 256), BF16),
            pltpu.VMEM((512, 128), F32),
            pltpu.VMEM((4, 64, 128), F32),
            pltpu.VMEM((4, 4, 16, 128), F32),
            dma((4, 4)), dma((3,)), dma((len(ROUNDS),)), dma((len(ROUNDS),)), dma((4,)), dma((4,)), dma((3,)), dma((3,)),
            dma((1,)), dma((1,)), dma((1,)), dma((1,)), dma((4,)), dma((1,)),
            pltpu.SemaphoreType.REGULAR, pltpu.SemaphoreType.REGULAR,
        ],
        compiler_params=pltpu.CompilerParams(
            collective_id=0, has_side_effects=True, vmem_limit_bytes=60 * 1024 * 1024
        ),
    )(
        volume, step_weights, row_interp, col_interp, tf_table, materials.transpose(1, 2, 0), entry
    )


def solution(mesh):
    torus = Mesh(mesh.devices.reshape(2, 2, 2, 4, 4), AXES)
    return jax.shard_map(
        render,
        mesh=torus,
        in_specs=(
            P(AXES, None, None),
            P(VIEW, None, None),
            P(VIEW, None, None),
            P(VIEW, None, None),
            P(),
            P(None, None, DEPTH),
            P(VIEW, None, None),
        ),
        out_specs=P(VIEW, None, DEPTH, None),
        check_vma=False,
    )
```

```python
import jax
import jax.numpy as jnp
from jax import lax
from jax.experimental import pallas as pl
from jax.experimental.pallas import tpu as pltpu
from jax.sharding import Mesh
from jax.sharding import PartitionSpec as P

AXES = ("zh", "core", "zl", "y", "x")
VIEW = ("zh", "core")
DEPTH = ("zl", "y", "x")
MESH = pl.DeviceIdType.MESH
STEP_LENGTH = 2.0 / 256.0
LOG2E = 1.4426950408889634
LN2 = 0.6931471805599453
BF16 = jnp.bfloat16
F32 = jnp.float32


def split(value):
    high = value.astype(BF16)
    low = (value - high.astype(F32)).astype(BF16)
    return high, low


def dot_nt(lhs, rhs):
    return lax.dot_general(lhs, rhs, (((1,), (1,)), ((), ())), preferred_element_type=F32)


def softplus2(v):
    power = jnp.exp2(jnp.minimum(v, 64.0))
    grown = 1.0 + power
    return jnp.maximum(v, jnp.log2(grown) + LOG2E * (power - (grown - 1.0)))


def step_block(weights):
    twice = jnp.concatenate([weights, weights], axis=1)
    lane = lax.broadcasted_iota(jnp.int32, twice.shape, 1)
    block = jnp.concatenate(
        [jnp.where(lane < 64, twice, 0.0), jnp.where(lane >= 64, twice, 0.0)], axis=0
    )
    high = block.astype(BF16).astype(F32)
    return high, block - high


def step_lhs(weights):
    parts = [step_block(one) for one in weights]
    high = jnp.concatenate([part[0] for part in parts], axis=0)
    low = jnp.concatenate([part[1] for part in parts], axis=0)
    top = jnp.concatenate([high, high], axis=1)
    bottom = jnp.concatenate([low, jnp.zeros_like(low)], axis=1)
    return jnp.concatenate([top, bottom], axis=0).astype(BF16)


ROUNDS = ((0, 2), (2, 2), (4, 1), (5, 1), (6, 1), (7, 1))


def kernel(
    vol, step_map, rows_map, cols_map, table_in, mats_in, entry, out,
    cells, sent, got, weights, table, mats, row_buf, col_buf, entry_buf, coef_own, coef_relay, coefs,
    row_lhs, col_rhs, second, samples, part, finals,
    cell_sem, small_sem, send_sem, got_sem, w_send, w_got, map_send, map_got,
    coef_send, coef_got, pair_send, pair_got, fin_send, fin_got, row_ready, plane_ready,
):
    zh, core, zl = lax.axis_index("zh"), lax.axis_index("core"), lax.axis_index("zl")
    y, x = lax.axis_index("y"), lax.axis_index("x")

    def cell_copy(rho, q):
        return pltpu.make_async_copy(
            vol.at[:, :, pl.ds(512 * q + 128 * rho, 128)], cells.at[rho, q], cell_sem.at[rho, q]
        )

    small = [
        pltpu.make_async_copy(step_map.at[0], weights.at[0], small_sem.at[0]),
        pltpu.make_async_copy(mats_in, mats, small_sem.at[1]),
        pltpu.make_async_copy(table_in, table, small_sem.at[2]),
    ]
    for copy in small:
        copy.start()

    place = y * 4 + x
    shift = lax.rem(y - 2 * core - zl + 8, 4)
    mine = lax.rem(2 + 3 * shift, 4)
    view_zh, view_core = lax.rem(zh + mine // 2, 2), lax.rem(core + lax.rem(mine, 2), 2)
    out_y = 2 * core + zl

    def device(zh_=zh, core_=core, zl_=zl, y_=y, x_=x):
        return {"zh": zh_, "core": core_, "zl": zl_, "y": y_, "x": x_}

    def remote(src, dst, send, recv, where):
        return pltpu.make_async_remote_copy(
            src_ref=src, dst_ref=dst, send_sem=send, recv_sem=recv,
            device_id=where, device_id_type=MESH,
        )

    def view_peer(xor):
        return device(zh_=lax.rem(zh + xor // 2, 2), core_=lax.rem(core + xor % 2, 2))

    def take(ref, sem):
        pltpu.make_async_copy(ref, ref, sem).wait()

    brick_slot = lax.rem(y, 2) * 4 + x
    coef_self = lax.rem(x, 2) == y // 2
    barrier = pltpu.get_barrier_semaphore()

    def greet(where):
        pl.semaphore_signal(barrier, inc=1, device_id=where, device_id_type=MESH)

    rows = [device(x_=lax.rem(x + i, 4)) for i in (2, 1, 3)]
    columns = [device(y_=lax.rem(y + i, 4)) for i in (2, 1, 3)]
    pair = device(zl_=1 - zl)
    with jax.named_scope("greet"):
        for peer in [view_peer(2), view_peer(3)] + rows + columns + [pair, view_peer(1)]:
            greet(peer)
    for rho in range(4):
        for q in range(4):
            cell_copy(rho, q).start()

    def contract(lhs, rho, q, first_view, count):
        high, low = split(cells[rho, q].reshape(512, 128))
        wide = dot_nt(lhs, jnp.concatenate([high, low], axis=1))
        wide = wide[: 16 * count] + wide[16 * count :]
        for k in range(count):
            for pair in range(2):
                for z in range(4):
                    row = 16 * k + 8 * pair
                    sent[(first_view + k) * 4 + q, 2 * rho + pair, pl.ds(8 * z, 8), :] = wide[
                        row : row + 8, 128 * z : 128 * z + 128
                    ]

    def plane_copy(xor, column, first, count, sem):
        peer_y = lax.rem((2 + 3 * xor) % 4 + 2 * core + zl, 4)
        copy = remote(
            sent.at[4 * xor + column, pl.ds(first, count)],
            got.at[pl.ds(first, count), pl.ds(pl.multiple_of(32 * place, 32), 32)],
            send_sem.at[sem], got_sem.at[sem], device(y_=peer_y, x_=column),
        )
        pl.when(jnp.logical_not((mine == xor) & (x == column)))(copy.start)

    def send_round(number, columns=range(4)):
        for xor in range(4):
            for column in columns:
                plane_copy(xor, column, *ROUNDS[number], number)

    def sent_round(number):
        first, count = ROUNDS[number]
        take(sent.at[pl.ds(0, 15), pl.ds(first, count)], send_sem.at[number])

    def send_coefs(plane, source):
        column = plane * 2 + y // 2
        for row in range(4):
            here = (row == y) & (column == x)
            copy = remote(
                source, coefs.at[brick_slot], coef_send.at[0], coef_got.at[0],
                device(y_=row, x_=column),
            )
            pl.when(jnp.logical_not(here))(copy.start)

            @pl.when(here)
            def _():
                coefs[brick_slot] = source[...]

    partner_copy = remote(
        coef_own.at[1 - zl], coef_relay, pair_send.at[0], pair_got.at[0], pair
    )
    w_copies = [
        remote(weights.at[0], weights.at[xor], w_send.at[xor], w_got.at[xor], view_peer(xor))
        for xor in (1, 2, 3)
    ]
    with jax.named_scope("small"):
        small[0].wait()
    with jax.named_scope("meet"):
        pl.semaphore_wait(barrier, 10)
    for copy in w_copies:
        copy.start()
    for peer in columns:
        pl.semaphore_signal(row_ready, inc=1, device_id=peer, device_id_type=MESH)
    with jax.named_scope("classes"):
        for copy in small[1:]:
            copy.wait()
        lane = lax.broadcasted_iota(jnp.int32, (8, 128), 1)
        sublane = lax.broadcasted_iota(jnp.int32, (8, 128), 0)
        for k in range(2):
            tile = 2 * (2 * zh + core) + k
            wanted = jnp.where(lane < 64, mats[0, 0, tile], mats[1, 0, tile])
            onehot = (sublane == wanted).astype(F32)
            coef_own[k] = lax.dot_general(
                table[...], onehot, (((0,), (0,)), ((), ())),
                precision=lax.Precision.HIGHEST, preferred_element_type=F32,
            )
        partner_copy.start()
    own_lhs = step_lhs([weights[0]])

    def own_view(rho):
        with jax.named_scope("wait_cells"):
            for q in range(4):
                cell_copy(rho, q).wait()
        with jax.named_scope("own_view"):
            for q in range(4):
                contract(own_lhs, rho, q, 0, 1)

    own_view(0)
    own_view(1)
    with jax.named_scope("plane"):
        pl.semaphore_wait(row_ready, 3)
    pl.semaphore_signal(plane_ready, inc=1, device_id=pair, device_id_type=MESH)
    send_coefs(zl, coef_own.at[zl])
    own_view(2)
    own_view(3)
    to_xor = jnp.where(lax.rem(shift, 2) == 1, lax.rem(2 + 3 * (shift + 2), 4), mine)
    to_zh, to_core = lax.rem(zh + to_xor // 2, 2), lax.rem(core + lax.rem(to_xor, 2), 2)
    to_rows = pl.multiple_of((2 * (2 * to_zh + to_core) + zl) * 64, 64)
    to_device = device(zh_=to_zh, core_=to_core)
    maps = (
        (rows_map.at[0], row_buf),
        (cols_map.at[0], col_buf),
        (entry.at[0, pl.ds(to_rows, 64)], entry_buf),
    )

    with jax.named_scope("relay"):
        partner_copy.wait()
        send_coefs(1 - zl, coef_relay)
    with jax.named_scope("wait_weights"):
        for copy in w_copies:
            copy.wait()
    lhs = step_lhs([weights[xor] for xor in (1, 2, 3)])
    for rho in range(4):
        with jax.named_scope("contract"):
            for i in range(4):
                q = lax.rem(x + i, 4) if rho == 0 else i
                contract(lhs, rho, q, 1, 3)
                if rho == 0:
                    send_round(0, (q,))
        if rho > 0:
            with jax.named_scope("send_round"):
                for number, (first, count) in enumerate(ROUNDS):
                    if (first + count - 1) // 2 == rho:
                        send_round(number)

    pl.semaphore_wait(plane_ready, 1)

    @pl.when(mine == 0)
    def _():
        for i, (src, dst) in enumerate(maps):
            pltpu.make_async_copy(src, dst, map_got.at[i]).start()

    @pl.when(mine != 0)
    def _():
        for i, (src, dst) in enumerate(maps):
            remote(src, dst, map_send.at[i], map_got.at[i], to_device).start()

    own_slot = 4 * mine + x

    @pl.loop(0, 8)
    def _(j):
        got[j, pl.ds(pl.multiple_of(32 * place, 32), 32), :] = sent[own_slot, j]

    with jax.named_scope("wait_maps"):
        for i, (src, dst) in enumerate(maps):
            pltpu.make_async_copy(src, dst, map_got.at[i]).wait()

    row_map = row_buf[...]
    row_high = row_map.astype(BF16).astype(F32)
    row_lhs[...] = jnp.concatenate([row_high, row_high, row_map - row_high], axis=1).astype(BF16)
    col_map = col_buf[...]
    none = jnp.zeros_like(col_map)
    col_block = jnp.concatenate(
        [jnp.concatenate([col_map, none], axis=1), jnp.concatenate([none, col_map], axis=1)], axis=0
    )
    col_high, col_low = split(col_block)
    col_rhs[...] = jnp.concatenate(
        [
            jnp.concatenate([col_high, col_high], axis=1),
            jnp.concatenate([col_low, jnp.zeros_like(col_low)], axis=1),
        ],
        axis=0,
    )

    def coef_done(sem):
        pl.when(coef_self)(lambda: take(coefs.at[pl.ds(0, 7)], sem))
        pl.when(jnp.logical_not(coef_self))(lambda: take(coefs, sem))

    with jax.named_scope("wait_classes"):
        coef_done(coef_got.at[0])

    part[0:3] = jnp.zeros((3, 64, 128), F32)
    part[3] = jnp.ones((64, 128), F32)

    def sample_brick(j):
        for pair in range(4):
            both = jnp.concatenate(
                [got[j, pl.ds(2 * pair + k, 64, stride=8), :] for k in range(2)], axis=1
            )
            high, low = split(both)
            rows = jnp.dot(
                row_lhs[...], jnp.concatenate([high, low, high], axis=0), preferred_element_type=F32
            )
            for k in range(2):
                high, low = split(rows[:, 128 * k : 128 * k + 128])
                at = pl.ds((2 * pair + k) * 64, 64)
                second[at, 0:128] = high
                second[at, 128:256] = low
        wide = dot_nt(second[...], col_rhs[...])
        samples[...] = wide[:, 0:128] + wide[:, 128:256]

    def shade(j, at):
        coef = LOG2E * coefs[j]
        rows = pl.ds(at, 32)
        opacity = jnp.where(entry_buf[rows, :] <= 8 * x + j, -STEP_LENGTH, 0.0)
        red, green, blue, through = part[0, rows], part[1, rows], part[2, rows], part[3, rows]
        for s in range(8):
            value = samples[pl.ds(at + 64 * s, 32), :]
            after = through * jnp.exp2(opacity * softplus2(coef[6:7] * value + coef[7:8]))
            weight = through - after
            through = after
            red = red + weight * softplus2(coef[0:1] * value + coef[3:4])
            green = green + weight * softplus2(coef[1:2] * value + coef[4:5])
            blue = blue + weight * softplus2(coef[2:3] * value + coef[5:6])
        part[0, rows], part[1, rows], part[2, rows], part[3, rows] = red, green, blue, through

    def final_copy(i):
        return remote(
            part.at[:, pl.ds(16 * i, 16)], finals.at[x], fin_send.at[i], fin_got.at[0],
            device(view_zh, view_core, zh, out_y, i),
        )

    for number, (first, count) in enumerate(ROUNDS):
        with jax.named_scope("wait_brick"):
            take(got.at[pl.ds(first, count), pl.ds(0, 480)], got_sem.at[number])
        with jax.named_scope("bricks"):
            @pl.loop(first, first + count)
            def _(j):
                sample_brick(j)
                if first + count < 8:
                    pl.loop(0, 2)(lambda block: shade(j, pl.multiple_of(block * 32, 32)))
                else:
                    for block in range(2):
                        shade(j, 32 * block)
                        final_copy(2 * block).start()
                        final_copy(2 * block + 1).start()

    with jax.named_scope("drain"):
        for number in range(len(ROUNDS)):
            sent_round(number)

    @pl.when(mine != 0)
    def _():
        for i, (src, dst) in enumerate(maps):
            remote(src, dst, map_send.at[i], map_got.at[i], to_device).wait_send()

    coef_done(coef_send.at[0])

    with jax.named_scope("wait_finals"):
        take(finals, fin_got.at[0])
    total = finals[3, 0:3]
    for q in (2, 1, 0):
        total = finals[q, 0:3] + finals[q, 3:4] * total
    out[0] = LN2 * total

    for i in range(4):
        final_copy(i).wait_send()


def render(volume, step_weights, row_interp, col_interp, tf_table, materials, entry):
    vmem = pl.BlockSpec(memory_space=pltpu.VMEM)
    anywhere = pl.BlockSpec(memory_space=pl.ANY)
    dma = pltpu.SemaphoreType.DMA
    return pl.pallas_call(
        kernel,
        name="render",
        out_shape=pltpu.VMEM((1, 3, 16, 128), F32),
        in_specs=[anywhere] * 7,
        out_specs=vmem,
        scratch_shapes=[
            pltpu.VMEM((4, 4, 4, 128, 128), F32),
            pltpu.VMEM((16, 8, 32, 128), F32),
            pltpu.VMEM((8, 512, 128), F32),
            pltpu.VMEM((4, 8, 64), F32),
            pltpu.VMEM((8, 8), F32),
            pltpu.SMEM((2, 1, 8), jnp.int32),
            pltpu.VMEM((64, 64), F32),
            pltpu.VMEM((64, 64), F32),
            pltpu.VMEM((64, 128), jnp.int32),
            pltpu.VMEM((2, 8, 128), F32),
            pltpu.VMEM((8, 128), F32),
            pltpu.VMEM((8, 8, 128), F32),
            pltpu.VMEM((64, 192), BF16),
            pltpu.VMEM((256, 256), BF16),
            pltpu.VMEM((512, 256), BF16),
            pltpu.VMEM((512, 128), F32),
            pltpu.VMEM((4, 64, 128), F32),
            pltpu.VMEM((4, 4, 16, 128), F32),
            dma((4, 4)), dma((3,)), dma((len(ROUNDS),)), dma((len(ROUNDS),)), dma((4,)), dma((4,)), dma((3,)), dma((3,)),
            dma((1,)), dma((1,)), dma((1,)), dma((1,)), dma((4,)), dma((1,)),
            pltpu.SemaphoreType.REGULAR, pltpu.SemaphoreType.REGULAR,
        ],
        compiler_params=pltpu.CompilerParams(
            collective_id=0, has_side_effects=True, vmem_limit_bytes=60 * 1024 * 1024
        ),
    )(
        volume, step_weights, row_interp, col_interp, tf_table, materials.transpose(1, 2, 0), entry
    )


def solution(mesh):
    torus = Mesh(mesh.devices.reshape(2, 2, 2, 4, 4), AXES)
    return jax.shard_map(
        render,
        mesh=torus,
        in_specs=(
            P(AXES, None, None),
            P(VIEW, None, None),
            P(VIEW, None, None),
            P(VIEW, None, None),
            P(),
            P(None, None, DEPTH),
            P(VIEW, None, None),
        ),
        out_specs=P(VIEW, None, DEPTH, None),
        check_vma=False,
    )
```
